32 devices in a mesh: turn: 4 (over y, core), blk: 4 (over z), strip: 2 (over x).
Axes of the slice: x: 2, y: 2, z: 4, core: 2. Of those that a mesh axis runs over, the one named last changes fastest.
Arguments:
- echoes: bfloat16 [2, 256, 32768], P(None, 'blk', ('turn', 'strip')), may hold values from -6 to 6
- filters: bfloat16 [2, 8, 32768], P(None, 'blk'), may hold values from -6 to 6
- slab_index: int32 [256], P(('blk', 'turn')), may hold values from 0 to 7
- shifts: int32 [256], P(('blk', 'turn')), may hold values from 0 to 32767
Outputs:
- focused: float32 [2, 256, 32768], P(None, ('blk', 'turn'), 'strip')
The draws below stay inside these ranges and needn't reach their ends.
All inputs are finite; a program needn't handle non-finite values.
Results may differ from the reference program's by a relative error of at most 0.0003.
Values may be sent and summed in bfloat16 or wider, within the bound.
A program may use at most 128 MiB of HBM per device.

```python
import jax
import jax.numpy as jnp
from jax import lax

NA = 32768
NR = 256
NS = 8


def plant(entries, stream_key, smallest, largest):
    dims = entries.shape
    place = [jax.random.randint(jax.random.fold_in(stream_key, axis), (), 0, dims[axis]) for axis in range(len(dims))]
    entries = entries.at[tuple(place)].set(smallest)
    longest = dims.index(max(dims))
    place[longest] = (place[longest] + 1) % dims[longest]
    return entries.at[tuple(place)].set(largest)


def block_scale(own_key, extent, split, smallest, high):
    loudness, own = 1.0, jax.random.fold_in(own_key, 6)
    for dim, blocks in split:
        steps = jnp.exp(jax.random.uniform(jax.random.fold_in(own, dim), (blocks,), jnp.float32, smallest / len(split), high / len(split)))
        loudness = loudness * jnp.repeat(steps, extent[dim] // blocks).reshape([-1 if axis == dim else 1 for axis in range(len(extent))])
    return loudness


def scatter_about(rng, shape, scale, limit, split=(), kind=jnp.bfloat16):
    values = jax.random.normal(rng, shape, jnp.float32) * scale
    if len(split) > 0:
        values = block_scale(rng, shape, split, -0.22, 0.18) * values
    return jnp.clip(values, min=-limit, max=limit).astype(kind)


def setup_inputs(seed: int = 0) -> dict:
    key_of = jax.random.split(jax.random.key(seed), 5)
    echoes = scatter_about(key_of[0], (2, NR, NA), 1.0, 6.0, ((1, 4), (2, 8)))
    filters = scatter_about(key_of[1], (2, NS, NA), 1.0, 6.0, ((1, 4),))
    slab_index = plant(jax.random.randint(key_of[2], (NR,), 0, NS), jax.random.fold_in(key_of[2], 1), 0, NS - 1).astype(jnp.int32)
    shifts = plant(jax.random.randint(key_of[3], (NR,), 0, NA), jax.random.fold_in(key_of[3], 1), 0, NA - 1).astype(jnp.int32)
    return dict(echoes=echoes, filters=filters, slab_index=slab_index, shifts=shifts)


def reference(echoes, filters, slab_index, shifts):
    signal = lax.complex(echoes[0].astype(jnp.float32), echoes[1].astype(jnp.float32))
    spectrum = jnp.fft.fft(signal, axis=1)
    chosen = lax.complex(filters[0][slab_index].astype(jnp.float32), filters[1][slab_index].astype(jnp.float32))
    image = jnp.fft.ifft(spectrum * chosen, axis=1)
    positions = (jnp.arange(NA, dtype=jnp.int32)[None, :] - shifts[:, None].astype(jnp.int32)) % NA
    rolled = jnp.take_along_axis(image, positions, axis=1)
    return jnp.stack([jnp.real(rolled), jnp.imag(rolled)]).astype(jnp.float32)
```

```python
import functools
import math

import jax
import jax.numpy as jnp
import numpy as np
from jax import lax
from jax.experimental import pallas as pl
from jax.experimental.pallas import tpu as pltpu
from jax.sharding import PartitionSpec as P

LANES = 128
PAIR = 2
MESH = pl.DeviceIdType.MESH
f32, bf16 = jnp.float32, jnp.bfloat16


def split_np(table):
    high = table.astype(jnp.bfloat16)
    low = (table - high.astype(np.float64)).astype(jnp.bfloat16)
    return high, low


def make_tables(length, sources, strips):
    half = LANES
    outer = length // (2 * half)
    local = outer // sources
    a_ids, c_ids = np.arange(outer), np.arange(outer)
    b_ids = np.arange(half)
    tau = np.exp(-2j * np.pi * half * c_ids / length)
    first = np.exp(-2j * np.pi * ((c_ids[:, None] * a_ids[None, :]) % outer) / outer)
    stage_one = []
    for mat in (first, tau[:, None] * first):
        grouped = mat.reshape(outer, sources, 1, local)
        top = np.concatenate([grouped.real, -grouped.imag], 2).reshape(outer, 2 * outer)
        bottom = np.concatenate([grouped.imag, grouped.real], 2).reshape(outer, 2 * outer)
        stage_one.append(np.concatenate(split_np(np.concatenate([top, bottom], 0)), 0))
    stage_one = np.stack(stage_one)
    base = np.exp(-2j * np.pi * ((b_ids[:, None] * b_ids[None, :]) % half) / half)

    def right(mat):
        whole = np.concatenate(
            [np.concatenate([mat.real, mat.imag], 1), np.concatenate([-mat.imag, mat.real], 1)], 0
        )
        high, low = split_np(whole)
        return np.concatenate([high, low, high], 0)

    stage_two = np.stack([right(base), right(base.conj())])
    twist = np.exp(-2j * np.pi * ((c_ids[:, None] * b_ids[None, :]) % length) / length)
    omega = np.exp(-2j * np.pi * b_ids / (2 * half))
    turned = twist * omega[None, :]
    twists = np.stack([twist.real, twist.imag, turned.real, turned.imag]).astype(np.float32)
    rows = outer // strips
    last = []
    for strip in range(strips):
        picked = np.arange(strip * rows, (strip + 1) * rows)
        back = np.exp(2j * np.pi * ((picked[:, None] * c_ids[None, :]) % outer) / outer) / length
        per_half = []
        for mat in (back, back * tau.conj()[None, :]):
            whole = np.concatenate(
                [np.concatenate([mat.real, -mat.imag], 1), np.concatenate([mat.imag, mat.real], 1)], 0
            )
            per_half.append(np.concatenate(split_np(whole), 0))
        last.append(np.stack(per_half))
    return stage_one, stage_two, twists, np.stack(last)


def cosine_sine(phase, length):
    quarter = length // 4
    wrapped = phase & (length - 1)
    quadrant = (wrapped + quarter // 2) // quarter if quarter & (quarter - 1) else (
        wrapped + quarter // 2
    ) >> (quarter.bit_length() - 1)
    angle = (wrapped - quadrant * quarter).astype(f32) * (2.0 * math.pi / length)
    square = angle * angle
    sine = angle * (
        1.0 + square * (-1.0 / 6 + square * (1.0 / 120 + square * (-1.0 / 5040 + square * (1.0 / 362880))))
    )
    cosine = 1.0 + square * (
        -0.5
        + square * (1.0 / 24 + square * (-1.0 / 720 + square * (1.0 / 40320 - square * (1.0 / 3628800))))
    )
    odd = (quadrant & 1) == 1
    out_cos = jnp.where(odd, sine, cosine)
    out_sin = jnp.where(odd, cosine, sine)
    quad = quadrant & 3
    out_cos = jnp.where((quad == 1) | (quad == 2), -out_cos, out_cos)
    out_sin = jnp.where(quad >= 2, -out_sin, out_sin)
    return out_cos, out_sin


def cmul(ar, ai, br, bi):
    return ar * br - ai * bi, ar * bi + ai * br


def split(values):
    high = values.astype(bf16)
    return high, (values - high.astype(f32)).astype(bf16)


def dot(left, right):
    return jnp.dot(left, right, preferred_element_type=f32)


def body(
    turns, blks, strips, length,
    shifts_ref, slabs_ref, ech_ref, filt_ref, one_ref, two_ref, twist_ref, last_ref,
    out_ref,
    recv, filt_all, inv_twist, ramp, spec,
    send_sem, recv_sem, fsend, frecv, gsend, grecv,
):
    turn, blk, strip = lax.axis_index("turn"), lax.axis_index("blk"), lax.axis_index("strip")
    row_count = recv.shape[0]
    pairs = row_count // PAIR
    slab_local = filt_ref.shape[0]
    core = lax.rem(turn, 2)
    partner = turn + 1 - 2 * core
    peers = [(dt, ds) for dt in range(turns) for ds in range(strips) if (dt, ds) != (0, 0)]

    def peer(dt, ds):
        return (lax.rem(turn + dt, turns), blk, lax.rem(strip + ds, strips))

    barrier = pltpu.get_barrier_semaphore()
    for dt, ds in peers:
        pl.semaphore_signal(barrier, inc=1, device_id=peer(dt, ds), device_id_type=MESH)
    for dz in range(1, blks):
        pl.semaphore_signal(
            barrier, inc=1, device_id=(turn, lax.rem(blk + dz, blks), strip), device_id_type=MESH
        )
    pl.semaphore_wait(barrier, len(peers) + blks - 1)

    me = turn * strips + strip

    def echo_copy(step, dt, ds):
        to = peer(dt, ds)
        return pltpu.make_async_remote_copy(
            src_ref=ech_ref.at[pl.ds(to[0] * row_count + step * PAIR, PAIR)],
            dst_ref=recv.at[pl.ds(step * PAIR, PAIR), me],
            send_sem=send_sem.at[step, dt * strips + ds],
            recv_sem=recv_sem.at[step, dt * strips + ds],
            device_id=to,
            device_id_type=MESH,
        )

    def filter_copy(dz):
        return pltpu.make_async_remote_copy(
            src_ref=filt_ref.at[:, core],
            dst_ref=filt_all.at[pl.ds(blk * slab_local, slab_local), core],
            send_sem=fsend.at[dz],
            recv_sem=frecv.at[dz],
            device_id=(turn, lax.rem(blk + dz, blks), strip),
            device_id_type=MESH,
        )

    def relay_copy(dz):
        origin = lax.rem(blk + blks - dz, blks)
        place = filt_all.at[pl.ds(origin * slab_local, slab_local), core]
        return pltpu.make_async_remote_copy(
            src_ref=place,
            dst_ref=place,
            send_sem=gsend.at[dz],
            recv_sem=grecv.at[dz],
            device_id=(partner, blk, strip),
            device_id_type=MESH,
        )

    for dz in range(1, blks):
        filter_copy(dz).start()

    def start_step(step, carry):
        for dt, ds in peers:
            echo_copy(step, dt, ds).start()
        return carry

    lax.fori_loop(0, pairs, start_step, 0)

    recv[:, me] = ech_ref[pl.ds(turn * row_count, row_count)]
    filt_all[pl.ds(blk * slab_local, slab_local)] = filt_ref[...]

    half = LANES
    outer = length // (2 * half)
    c_ids = lax.broadcasted_iota(jnp.int32, (outer, half), 0)
    lane_ids = lax.broadcasted_iota(jnp.int32, (8, 2 * half), 1)
    k_ids = jnp.where(lane_ids >= half, (lane_ids - half) * (2 * outer) + outer, lane_ids * (2 * outer))

    def prepare(row, carry):
        shift = shifts_ref[row]
        vr, vi = cosine_sine(c_ids * shift, length)
        vi = -vi
        for part in range(2):
            tr, ti = twist_ref[2 * part], -twist_ref[2 * part + 1]
            rr, ri = cmul(tr, ti, vr, vi)
            inv_twist[row, 2 * part] = rr
            inv_twist[row, 2 * part + 1] = ri
        ur, ui = cosine_sine(k_ids * shift, length)
        ramp[row, 0] = ur
        ramp[row, 1] = -ui
        return carry

    lax.fori_loop(0, row_count, prepare, 0)

    def lefts(blocks):
        highs, lows = [], []
        for re, im in blocks:
            high, low = split(jnp.concatenate([re, im], 1))
            highs.append(high)
            lows.append(low)
        high, low = jnp.concatenate(highs, 0), jnp.concatenate(lows, 0)
        return jnp.concatenate([high, high, low], 1)

    def forward(step, carry):
        for dt, ds in peers:
            echo_copy(step, dt, ds).wait_recv()
        rows = [recv[step * PAIR + i].reshape(2 * outer, 2 * half) for i in range(PAIR)]
        parts = []
        for side in range(2):
            lanes = slice(side * half, (side + 1) * half)
            res = dot(one_ref[side], jnp.concatenate([r[:, lanes] for r in rows], 1))
            parts.append(res[: 2 * outer] + res[2 * outer :])
        total, differ = parts[0] + parts[1], parts[0] - parts[1]
        blocks = []
        for e, value in enumerate((total, differ)):
            tr, ti = twist_ref[2 * e], twist_ref[2 * e + 1]
            for i in range(PAIR):
                lanes = slice(i * half, (i + 1) * half)
                blocks.append(cmul(value[:outer, lanes], value[outer:, lanes], tr, ti))
        spec[step] = dot(lefts(blocks), two_ref[0])
        return carry

    def inverse(step, carry):
        blocks = []
        for e in range(2):
            lanes = slice(e * half, (e + 1) * half)
            for i in range(PAIR):
                row = step * PAIR + i
                picked = filt_all[slabs_ref[row]].astype(f32)
                ur, ui = ramp[row, 0][:1, lanes], ramp[row, 1][:1, lanes]
                gr, gi = cmul(picked[0][:, lanes], picked[1][:, lanes], ur, ui)
                base = (e * PAIR + i) * outer
                z = spec[step, base : base + outer]
                blocks.append(cmul(z[:, :half], z[:, half:], gr, gi))
        back = dot(lefts(blocks), two_ref[1])
        lows, highs = [], []
        for i in range(PAIR):
            row = step * PAIR + i
            got = []
            for e in range(2):
                base = (e * PAIR + i) * outer
                u = back[base : base + outer]
                got.append(
                    cmul(u[:, :half], u[:, half:], inv_twist[row, 2 * e], inv_twist[row, 2 * e + 1])
                )
            lows.append(jnp.concatenate([got[0][0] + got[1][0], got[0][1] + got[1][1]], 0))
            highs.append(jnp.concatenate([got[0][0] - got[1][0], got[0][1] - got[1][1]], 0))
        rows = outer // strips
        for side, value in enumerate((lows, highs)):
            high, low = split(jnp.concatenate(value, 1))
            left = last_ref[strip, side]
            res = dot(left, high)
            res = res[: 2 * rows] + res[2 * rows :] + dot(left[: 2 * rows], low)
            for i in range(PAIR):
                row = step * PAIR + i
                for part in range(2):
                    out_ref[part, row, :, side * half : (side + 1) * half] = res[
                        part * rows : (part + 1) * rows, i * half : (i + 1) * half
                    ]
        return carry

    def both(step, carry):
        forward(step, 0)
        inverse(step, 0)
        return carry

    early = pairs // 2
    lax.fori_loop(0, early, forward, 0)
    for dz in range(1, blks):
        filter_copy(dz).wait_recv()
        relay_copy(dz).start()
    for dz in range(1, blks):
        relay_copy(dz).wait_recv()
    lax.fori_loop(0, early, inverse, 0)
    lax.fori_loop(early, pairs, both, 0)

    def end_step(step, carry):
        for dt, ds in peers:
            echo_copy(step, dt, ds).wait_send()
        return carry

    lax.fori_loop(0, pairs, end_step, 0)
    for dz in range(1, blks):
        filter_copy(dz).wait_send()
        relay_copy(dz).wait_send()


def per_device(turns, blks, strips, echoes, filters, slab_index, shifts):
    sources = turns * strips
    length = filters.shape[2]
    half = LANES
    outer = length // (2 * half)
    local = outer // sources
    row_count = slab_index.shape[0]
    slab_local = filters.shape[1]
    pairs = row_count // PAIR
    shaped = echoes.transpose(1, 0, 2).reshape(-1, 2 * local, 2 * half)
    response = (
        filters.reshape(2, slab_local, half, 2, outer)
        .transpose(1, 0, 4, 3, 2)
        .reshape(slab_local, 2, outer, 2 * half)
    )
    tables = [jnp.asarray(t) for t in make_tables(length, sources, strips)]
    vmem, smem = pl.BlockSpec(memory_space=pltpu.VMEM), pl.BlockSpec(memory_space=pltpu.SMEM)
    rows = outer // strips
    image = pl.pallas_call(
        functools.partial(body, turns, blks, strips, length),
        out_shape=jax.ShapeDtypeStruct((2, row_count, rows, 2 * half), f32),
        in_specs=[smem, smem] + [vmem] * 6,
        out_specs=vmem,
        scratch_shapes=[
            pltpu.VMEM((row_count, sources, 2 * local, 2 * half), bf16),
            pltpu.VMEM((slab_local * blks, 2, outer, 2 * half), bf16),
            pltpu.VMEM((row_count, 4, outer, half), f32),
            pltpu.VMEM((row_count, 2, 8, 2 * half), f32),
            pltpu.VMEM((pairs, 2 * PAIR * outer, 2 * half), f32),
            pltpu.SemaphoreType.DMA((pairs, sources)),
            pltpu.SemaphoreType.DMA((pairs, sources)),
            pltpu.SemaphoreType.DMA((blks,)),
            pltpu.SemaphoreType.DMA((blks,)),
            pltpu.SemaphoreType.DMA((blks,)),
            pltpu.SemaphoreType.DMA((blks,)),
        ],
        compiler_params=pltpu.CompilerParams(
            collective_id=0, has_side_effects=True, vmem_limit_bytes=56 * 1024 * 1024
        ),
    )(shifts, slab_index, shaped, response, *tables)
    return image.reshape(2, row_count, rows * 2 * half)


def solution(mesh):
    in_specs = (
        P(None, "blk", ("turn", "strip")),
        P(None, "blk", None),
        P(("blk", "turn")),
        P(("blk", "turn")),
    )
    out_specs = P(None, ("blk", "turn"), "strip")
    local = functools.partial(
        per_device, mesh.shape["turn"], mesh.shape["blk"], mesh.shape["strip"]
    )
    return jax.shard_map(local, mesh=mesh, in_specs=in_specs, out_specs=out_specs, check_vma=False)
```

```python
import functools
import math

import jax
import jax.numpy as jnp
import numpy as np
from jax import lax
from jax.experimental import pallas as pl
from jax.experimental.pallas import tpu as pltpu
from jax.sharding import PartitionSpec as P

LANES = 128
PAIR = 2
MESH = pl.DeviceIdType.MESH
f32, bf16 = jnp.float32, jnp.bfloat16


def split_np(table):
    high = table.astype(jnp.bfloat16)
    low = (table - high.astype(np.float64)).astype(jnp.bfloat16)
    return high, low


def make_tables(length, sources, strips):
    half = LANES
    outer = length // (2 * half)
    local = outer // sources
    a_ids, c_ids = np.arange(outer), np.arange(outer)
    b_ids = np.arange(half)
    tau = np.exp(-2j * np.pi * half * c_ids / length)
    first = np.exp(-2j * np.pi * ((c_ids[:, None] * a_ids[None, :]) % outer) / outer)
    stage_one = []
    for mat in (first, tau[:, None] * first):
        grouped = mat.reshape(outer, sources, 1, local)
        top = np.concatenate([grouped.real, -grouped.imag], 2).reshape(outer, 2 * outer)
        bottom = np.concatenate([grouped.imag, grouped.real], 2).reshape(outer, 2 * outer)
        stage_one.append(np.concatenate(split_np(np.concatenate([top, bottom], 0)), 0))
    stage_one = np.stack(stage_one)
    base = np.exp(-2j * np.pi * ((b_ids[:, None] * b_ids[None, :]) % half) / half)

    def right(mat):
        whole = np.concatenate(
            [np.concatenate([mat.real, mat.imag], 1), np.concatenate([-mat.imag, mat.real], 1)], 0
        )
        high, low = split_np(whole)
        return np.concatenate([high, low, high], 0)

    stage_two = np.stack([right(base), right(base.conj())])
    twist = np.exp(-2j * np.pi * ((c_ids[:, None] * b_ids[None, :]) % length) / length)
    omega = np.exp(-2j * np.pi * b_ids / (2 * half))
    turned = twist * omega[None, :]
    twists = np.stack([twist.real, twist.imag, turned.real, turned.imag]).astype(np.float32)
    rows = outer // strips
    last = []
    for strip in range(strips):
        picked = np.arange(strip * rows, (strip + 1) * rows)
        back = np.exp(2j * np.pi * ((picked[:, None] * c_ids[None, :]) % outer) / outer) / length
        per_half = []
        for mat in (back, back * tau.conj()[None, :]):
            whole = np.concatenate(
                [np.concatenate([mat.real, -mat.imag], 1), np.concatenate([mat.imag, mat.real], 1)], 0
            )
            per_half.append(np.concatenate(split_np(whole), 0))
        last.append(np.stack(per_half))
    return stage_one, stage_two, twists, np.stack(last)


def cosine_sine(phase, length):
    quarter = length // 4
    wrapped = phase & (length - 1)
    quadrant = (wrapped + quarter // 2) // quarter if quarter & (quarter - 1) else (
        wrapped + quarter // 2
    ) >> (quarter.bit_length() - 1)
    angle = (wrapped - quadrant * quarter).astype(f32) * (2.0 * math.pi / length)
    square = angle * angle
    sine = angle * (
        1.0 + square * (-1.0 / 6 + square * (1.0 / 120 + square * (-1.0 / 5040 + square * (1.0 / 362880))))
    )
    cosine = 1.0 + square * (
        -0.5
        + square * (1.0 / 24 + square * (-1.0 / 720 + square * (1.0 / 40320 - square * (1.0 / 3628800))))
    )
    odd = (quadrant & 1) == 1
    out_cos = jnp.where(odd, sine, cosine)
    out_sin = jnp.where(odd, cosine, sine)
    quad = quadrant & 3
    out_cos = jnp.where((quad == 1) | (quad == 2), -out_cos, out_cos)
    out_sin = jnp.where(quad >= 2, -out_sin, out_sin)
    return out_cos, out_sin


def cmul(ar, ai, br, bi):
    return ar * br - ai * bi, ar * bi + ai * br


def split(values):
    high = values.astype(bf16)
    return high, (values - high.astype(f32)).astype(bf16)


def dot(left, right):
    return jnp.dot(left, right, preferred_element_type=f32)


def body(
    turns, blks, strips, length,
    shifts_ref, slabs_ref, ech_ref, filt_ref, one_hbm, two_hbm, twist_hbm, last_hbm,
    out_hbm,
    recv, filt_all, inv_twist, ramp, spec, one_ref, two_ref, twist_ref, last_ref, out_ref,
    send_sem, recv_sem, fsend, frecv, gsend, grecv, own_sem, out_sem, load_sem,
):
    turn, blk, strip = lax.axis_index("turn"), lax.axis_index("blk"), lax.axis_index("strip")
    pairs = recv.shape[0]
    row_count = pairs * PAIR
    slab_local = filt_ref.shape[0]
    core = lax.rem(turn, 2)
    partner = turn + 1 - 2 * core
    peers = [(dt, ds) for dt in range(turns) for ds in range(strips) if (dt, ds) != (0, 0)]

    def peer(dt, ds):
        return (lax.rem(turn + dt, turns), blk, lax.rem(strip + ds, strips))

    me = turn * strips + strip
    twist_load = pltpu.make_async_copy(twist_hbm, twist_ref, load_sem.at[0])
    one_load = pltpu.make_async_copy(one_hbm, one_ref, load_sem.at[1])
    two_load = pltpu.make_async_copy(two_hbm, two_ref, load_sem.at[2])
    last_load = pltpu.make_async_copy(last_hbm.at[strip], last_ref, load_sem.at[3])
    filter_load = pltpu.make_async_copy(
        filt_ref, filt_all.at[pl.ds(blk * slab_local, slab_local)], load_sem.at[4]
    )

    def own_copy(step):
        return pltpu.make_async_copy(
            ech_ref.at[:, pl.ds(turn * row_count + step * PAIR, PAIR)],
            recv.at[step, me],
            own_sem.at[step],
        )

    def out_copy(step):
        group = step // (8 // PAIR)
        return pltpu.make_async_copy(out_ref.at[:, group], out_hbm.at[:, group], out_sem.at[group])

    barrier = pltpu.get_barrier_semaphore()
    for dt, ds in peers:
        pl.semaphore_signal(barrier, inc=1, device_id=peer(dt, ds), device_id_type=MESH)
    for dz in range(1, blks):
        pl.semaphore_signal(
            barrier, inc=1, device_id=(turn, lax.rem(blk + dz, blks), strip), device_id_type=MESH
        )
    twist_load.start()
    one_load.start()
    two_load.start()
    last_load.start()
    filter_load.start()
    pl.semaphore_wait(barrier, len(peers) + blks - 1)

    def echo_copy(step, dt, ds):
        to = peer(dt, ds)
        return pltpu.make_async_remote_copy(
            src_ref=ech_ref.at[:, pl.ds(to[0] * row_count + step * PAIR, PAIR)],
            dst_ref=recv.at[step, me],
            send_sem=send_sem.at[step, dt * strips + ds],
            recv_sem=recv_sem.at[step, dt * strips + ds],
            device_id=to,
            device_id_type=MESH,
        )

    def filter_copy(dz):
        return pltpu.make_async_remote_copy(
            src_ref=filt_ref.at[:, core],
            dst_ref=filt_all.at[pl.ds(blk * slab_local, slab_local), core],
            send_sem=fsend.at[dz],
            recv_sem=frecv.at[dz],
            device_id=(turn, lax.rem(blk + dz, blks), strip),
            device_id_type=MESH,
        )

    def relay_copy(dz):
        origin = lax.rem(blk + blks - dz, blks)
        place = filt_all.at[pl.ds(origin * slab_local, slab_local), core]
        return pltpu.make_async_remote_copy(
            src_ref=place,
            dst_ref=place,
            send_sem=gsend.at[dz],
            recv_sem=grecv.at[dz],
            device_id=(partner, blk, strip),
            device_id_type=MESH,
        )

    for dz in range(1, blks):
        filter_copy(dz).start()

    def start_step(step, carry):
        for dt, ds in peers:
            echo_copy(step, dt, ds).start()
        own_copy(step).start()
        return carry

    lax.fori_loop(0, pairs, start_step, 0)

    half = LANES
    outer = length // (2 * half)
    c_ids = lax.broadcasted_iota(jnp.int32, (outer, half), 0)
    lane_ids = lax.broadcasted_iota(jnp.int32, (8, 2 * half), 1)
    k_ids = jnp.where(lane_ids >= half, (lane_ids - half) * (2 * outer) + outer, lane_ids * (2 * outer))

    def prepare(row, carry):
        shift = shifts_ref[row]
        vr, vi = cosine_sine(c_ids * shift, length)
        vi = -vi
        for part in range(2):
            tr, ti = twist_ref[2 * part], -twist_ref[2 * part + 1]
            rr, ri = cmul(tr, ti, vr, vi)
            inv_twist[row, 2 * part] = rr
            inv_twist[row, 2 * part + 1] = ri
        ur, ui = cosine_sine(k_ids * shift, length)
        ramp[row, 0] = ur
        ramp[row, 1] = -ui
        return carry

    twist_load.wait()
    lax.fori_loop(0, row_count, prepare, 0)
    one_load.wait()
    two_load.wait()

    def lefts(blocks):
        highs, lows = [], []
        for re, im in blocks:
            high, low = split(jnp.concatenate([re, im], 1))
            highs.append(high)
            lows.append(low)
        high, low = jnp.concatenate(highs, 0), jnp.concatenate(lows, 0)
        return jnp.concatenate([high, high, low], 1)

    def forward(step, carry):
        for dt, ds in peers:
            echo_copy(step, dt, ds).wait_recv()
        own_copy(step).wait()
        rows = [recv[step, :, :, i].reshape(2 * outer, 2 * half) for i in range(PAIR)]
        parts = []
        for side in range(2):
            lanes = slice(side * half, (side + 1) * half)
            res = dot(one_ref[side], jnp.concatenate([r[:, lanes] for r in rows], 1))
            parts.append(res[: 2 * outer] + res[2 * outer :])
        total, differ = parts[0] + parts[1], parts[0] - parts[1]
        blocks = []
        for e, value in enumerate((total, differ)):
            tr, ti = twist_ref[2 * e], twist_ref[2 * e + 1]
            for i in range(PAIR):
                lanes = slice(i * half, (i + 1) * half)
                blocks.append(cmul(value[:outer, lanes], value[outer:, lanes], tr, ti))
        spec[step] = dot(lefts(blocks), two_ref[0])
        return carry

    def inverse(step, carry):
        blocks = []
        for e in range(2):
            lanes = slice(e * half, (e + 1) * half)
            for i in range(PAIR):
                row = step * PAIR + i
                picked = filt_all[slabs_ref[row], :, e].astype(f32)
                ur, ui = ramp[row, 0][:1, lanes], ramp[row, 1][:1, lanes]
                gr, gi = cmul(picked[0], picked[1], ur, ui)
                base = (e * PAIR + i) * outer
                z = spec[step, base : base + outer]
                blocks.append(cmul(z[:, :half], z[:, half:], gr, gi))
        back = dot(lefts(blocks), two_ref[1])
        lows, highs = [], []
        for i in range(PAIR):
            row = step * PAIR + i
            got = []
            for e in range(2):
                base = (e * PAIR + i) * outer
                u = back[base : base + outer]
                got.append(
                    cmul(u[:, :half], u[:, half:], inv_twist[row, 2 * e], inv_twist[row, 2 * e + 1])
                )
            lows.append(jnp.concatenate([got[0][0] + got[1][0], got[0][1] + got[1][1]], 0))
            highs.append(jnp.concatenate([got[0][0] - got[1][0], got[0][1] - got[1][1]], 0))
        rows = outer // strips
        for side, value in enumerate((lows, highs)):
            high, low = split(jnp.concatenate(value, 1))
            left = last_ref[side]
            res = dot(left, high)
            res = res[: 2 * rows] + res[2 * rows :] + dot(left[: 2 * rows], low)
            for i in range(PAIR):
                place = lax.rem(step, 8 // PAIR) * PAIR + i + 8 * side
                for part in range(2):
                    out_ref[part, step // (8 // PAIR), pl.ds(place, rows, stride=16), :] = res[
                        part * rows : (part + 1) * rows, i * half : (i + 1) * half
                    ]
        return carry

    def both(step, carry):
        forward(step, 0)
        inverse(step, 0)
        return carry

    early = pairs // 2
    lax.fori_loop(0, early, forward, 0)
    for dz in range(1, blks):
        filter_copy(dz).wait_recv()
        relay_copy(dz).start()
    for dz in range(1, blks):
        relay_copy(dz).wait_recv()
    filter_load.wait()
    last_load.wait()
    lax.fori_loop(0, early, inverse, 0)
    groups = row_count // 8
    per_group = 8 // PAIR
    for group in range(groups):
        lax.fori_loop(max(early, group * per_group), max(early, (group + 1) * per_group), both, 0)
        out_copy(group * per_group).start()

    def end_step(step, carry):
        for dt, ds in peers:
            echo_copy(step, dt, ds).wait_send()
        return carry

    lax.fori_loop(0, pairs, end_step, 0)
    for dz in range(1, blks):
        filter_copy(dz).wait_send()
        relay_copy(dz).wait_send()
    for group in range(groups):
        out_copy(group * per_group).wait()


def per_device(turns, blks, strips, echoes, filters, slab_index, shifts):
    sources = turns * strips
    length = filters.shape[2]
    half = LANES
    outer = length // (2 * half)
    local = outer // sources
    row_count = slab_index.shape[0]
    slab_local = filters.shape[1]
    pairs = row_count // PAIR
    shaped = echoes.reshape(2, -1, local, 2 * half)
    response = filters.reshape(2, slab_local, half, 2, outer).transpose(1, 0, 3, 4, 2)
    tables = [jnp.asarray(t) for t in make_tables(length, sources, strips)]
    hbm, smem = pl.BlockSpec(memory_space=pl.ANY), pl.BlockSpec(memory_space=pltpu.SMEM)
    rows = outer // strips
    image = pl.pallas_call(
        functools.partial(body, turns, blks, strips, length),
        out_shape=jax.ShapeDtypeStruct((2, row_count // 8, rows * 16, half), f32),
        in_specs=[smem, smem] + [hbm] * 6,
        out_specs=hbm,
        scratch_shapes=[
            pltpu.VMEM((pairs, sources, 2, PAIR, local, 2 * half), bf16),
            pltpu.VMEM((slab_local * blks, 2, 2, outer, half), bf16),
            pltpu.VMEM((row_count, 4, outer, half), f32),
            pltpu.VMEM((row_count, 2, 8, 2 * half), f32),
            pltpu.VMEM((pairs, 2 * PAIR * outer, 2 * half), f32),
            pltpu.VMEM(tables[0].shape, bf16),
            pltpu.VMEM(tables[1].shape, bf16),
            pltpu.VMEM(tables[2].shape, f32),
            pltpu.VMEM(tables[3].shape[1:], bf16),
            pltpu.VMEM((2, row_count // 8, rows * 16, half), f32),
            pltpu.SemaphoreType.DMA((pairs, sources)),
            pltpu.SemaphoreType.DMA((pairs, sources)),
            pltpu.SemaphoreType.DMA((blks,)),
            pltpu.SemaphoreType.DMA((blks,)),
            pltpu.SemaphoreType.DMA((blks,)),
            pltpu.SemaphoreType.DMA((blks,)),
            pltpu.SemaphoreType.DMA((pairs,)),
            pltpu.SemaphoreType.DMA((row_count // 8,)),
            pltpu.SemaphoreType.DMA((5,)),
        ],
        compiler_params=pltpu.CompilerParams(
            collective_id=0, has_side_effects=True, vmem_limit_bytes=56 * 1024 * 1024
        ),
    )(shifts, slab_index, shaped, response, *tables)
    image = image.reshape(2, row_count // 8, rows * 2, 8, half).transpose(0, 1, 3, 2, 4)
    return image.reshape(2, row_count, rows * 2 * half)


def solution(mesh):
    in_specs = (
        P(None, "blk", ("turn", "strip")),
        P(None, "blk", None),
        P(("blk", "turn")),
        P(("blk", "turn")),
    )
    out_specs = P(None, ("blk", "turn"), "strip")
    local = functools.partial(
        per_device, mesh.shape["turn"], mesh.shape["blk"], mesh.shape["strip"]
    )
    return jax.shard_map(local, mesh=mesh, in_specs=in_specs, out_specs=out_specs, check_vma=False)
```

```python
import functools
import math

import jax
import jax.numpy as jnp
import numpy as np
from jax import lax
from jax.experimental import pallas as pl
from jax.experimental.pallas import tpu as pltpu
from jax.sharding import PartitionSpec as P

LANES = 128
PAIR = 2
MESH = pl.DeviceIdType.MESH
f32, bf16 = jnp.float32, jnp.bfloat16


def split_np(table):
    high = table.astype(jnp.bfloat16)
    low = (table - high.astype(np.float64)).astype(jnp.bfloat16)
    return high, low


def make_tables(length, sources, strips):
    half = LANES
    outer = length // (2 * half)
    local = outer // sources
    a_ids, c_ids = np.arange(outer), np.arange(outer)
    b_ids = np.arange(half)
    tau = np.exp(-2j * np.pi * half * c_ids / length)
    first = np.exp(-2j * np.pi * ((c_ids[:, None] * a_ids[None, :]) % outer) / outer)
    stage_one = []
    for mat in (first, tau[:, None] * first):
        grouped = mat.reshape(outer, sources, 1, local)
        top = np.concatenate([grouped.real, -grouped.imag], 2).reshape(outer, 2 * outer)
        bottom = np.concatenate([grouped.imag, grouped.real], 2).reshape(outer, 2 * outer)
        stage_one.append(np.concatenate(split_np(np.concatenate([top, bottom], 0)), 0))
    stage_one = np.stack(stage_one)
    base = np.exp(-2j * np.pi * ((b_ids[:, None] * b_ids[None, :]) % half) / half)

    def right(mat):
        whole = np.concatenate(
            [np.concatenate([mat.real, mat.imag], 1), np.concatenate([-mat.imag, mat.real], 1)], 0
        )
        high, low = split_np(whole)
        return np.concatenate([high, low, high], 0)

    stage_two = np.stack([right(base), right(base.conj())])
    twist = np.exp(-2j * np.pi * ((c_ids[:, None] * b_ids[None, :]) % length) / length)
    omega = np.exp(-2j * np.pi * b_ids / (2 * half))
    turned = twist * omega[None, :]
    twists = np.stack([twist.real, twist.imag, turned.real, turned.imag]).astype(np.float32)
    rows = outer // strips
    last = []
    for strip in range(strips):
        picked = np.arange(strip * rows, (strip + 1) * rows)
        back = np.exp(2j * np.pi * ((picked[:, None] * c_ids[None, :]) % outer) / outer) / length
        per_half = []
        for mat in (back, back * tau.conj()[None, :]):
            whole = np.concatenate(
                [np.concatenate([mat.real, -mat.imag], 1), np.concatenate([mat.imag, mat.real], 1)], 0
            )
            per_half.append(np.concatenate(split_np(whole), 0))
        last.append(np.stack(per_half))
    return stage_one, stage_two, twists, np.stack(last)


def cosine_sine(phase, length):
    quarter = length // 4
    wrapped = phase & (length - 1)
    quadrant = (wrapped + quarter // 2) // quarter if quarter & (quarter - 1) else (
        wrapped + quarter // 2
    ) >> (quarter.bit_length() - 1)
    angle = (wrapped - quadrant * quarter).astype(f32) * (2.0 * math.pi / length)
    square = angle * angle
    sine = angle * (
        1.0 + square * (-1.0 / 6 + square * (1.0 / 120 + square * (-1.0 / 5040 + square * (1.0 / 362880))))
    )
    cosine = 1.0 + square * (
        -0.5
        + square * (1.0 / 24 + square * (-1.0 / 720 + square * (1.0 / 40320 - square * (1.0 / 3628800))))
    )
    odd = (quadrant & 1) == 1
    out_cos = jnp.where(odd, sine, cosine)
    out_sin = jnp.where(odd, cosine, sine)
    quad = quadrant & 3
    out_cos = jnp.where((quad == 1) | (quad == 2), -out_cos, out_cos)
    out_sin = jnp.where(quad >= 2, -out_sin, out_sin)
    return out_cos, out_sin


def cmul(ar, ai, br, bi):
    return ar * br - ai * bi, ar * bi + ai * br


def split(values):
    high = values.astype(bf16)
    return high, (values - high.astype(f32)).astype(bf16)


def dot(left, right):
    return jnp.dot(left, right, preferred_element_type=f32)


def body(
    turns, blks, strips, length,
    shifts_ref, slabs_ref, ech_ref, filt_ref, one_hbm, two_hbm, twist_hbm, last_hbm,
    out_ref,
    recv, filt_all, inv_twist, ramp, spec, one_ref, two_ref, twist_ref, last_ref, ech_raw, filt_raw, staged, outbox,
    send_sem, recv_sem, fsend, frecv, gsend, grecv, load_sem,
):
    turn, blk, strip = lax.axis_index("turn"), lax.axis_index("blk"), lax.axis_index("strip")
    pairs = recv.shape[0]
    row_count = pairs * PAIR
    slab_local = filt_ref.shape[1] * LANES // length
    core = lax.rem(turn, 2)
    partner = turn + 1 - 2 * core
    peers = [(dt, ds) for dt in range(turns) for ds in range(strips) if (dt, ds) != (0, 0)]

    def peer(dt, ds):
        return (lax.rem(turn + dt, turns), blk, lax.rem(strip + ds, strips))

    me = turn * strips + strip
    twist_load = pltpu.make_async_copy(twist_hbm, twist_ref, load_sem.at[0])
    one_load = pltpu.make_async_copy(one_hbm, one_ref, load_sem.at[1])
    two_load = pltpu.make_async_copy(two_hbm, two_ref, load_sem.at[2])
    last_load = pltpu.make_async_copy(last_hbm.at[strip], last_ref, load_sem.at[3])
    echo_load = pltpu.make_async_copy(ech_ref, ech_raw, load_sem.at[4])
    filter_load = pltpu.make_async_copy(filt_ref, filt_raw, load_sem.at[5])
    echo_load.start()
    filter_load.start()

    barrier = pltpu.get_barrier_semaphore()
    for dt, ds in peers:
        pl.semaphore_signal(barrier, inc=1, device_id=peer(dt, ds), device_id_type=MESH)
    for dz in range(1, blks):
        pl.semaphore_signal(
            barrier, inc=1, device_id=(turn, lax.rem(blk + dz, blks), strip), device_id_type=MESH
        )
    twist_load.start()
    one_load.start()
    two_load.start()
    last_load.start()
    pl.semaphore_wait(barrier, len(peers) + blks - 1)

    def echo_copy(step, dt, ds):
        to = peer(dt, ds)
        return pltpu.make_async_remote_copy(
            src_ref=outbox.at[to[0], step],
            dst_ref=recv.at[step, me],
            send_sem=send_sem.at[step, dt * strips + ds],
            recv_sem=recv_sem.at[step, dt * strips + ds],
            device_id=to,
            device_id_type=MESH,
        )

    def filter_copy(dz):
        return pltpu.make_async_remote_copy(
            src_ref=filt_all.at[pl.ds(blk * slab_local, slab_local), core],
            dst_ref=filt_all.at[pl.ds(blk * slab_local, slab_local), core],
            send_sem=fsend.at[dz],
            recv_sem=frecv.at[dz],
            device_id=(turn, lax.rem(blk + dz, blks), strip),
            device_id_type=MESH,
        )

    def relay_copy(dz):
        origin = lax.rem(blk + blks - dz, blks)
        place = filt_all.at[pl.ds(origin * slab_local, slab_local), core]
        return pltpu.make_async_remote_copy(
            src_ref=place,
            dst_ref=place,
            send_sem=gsend.at[dz],
            recv_sem=grecv.at[dz],
            device_id=(partner, blk, strip),
            device_id_type=MESH,
        )

    half = LANES
    outer = length // (2 * half)
    local = ech_raw.shape[2] // 2
    groups = row_count // 8
    per_group = 8 // PAIR

    def arrange(group):
        def fill(to, carry):
            for part in range(2):
                values = ech_raw[part, to * groups + group].astype(f32)
                staged[part] = values.reshape(2 * local * 8, half)
            for part in range(2):
                for row in range(8):
                    for side in range(2):
                        value = staged[part, pl.ds(side * 8 + row, local, stride=16), :]
                        outbox[
                            to, group * per_group + row // PAIR, part, row % PAIR, :,
                            side * half : (side + 1) * half,
                        ] = value.astype(bf16)
            return carry

        lax.fori_loop(0, turns, fill, 0)
        first, end = group * per_group, (group + 1) * per_group

        def start_step(step, carry):
            for dt, ds in peers:
                echo_copy(step, dt, ds).start()
            return carry

        lax.fori_loop(first, end, start_step, 0)

        def keep(step, carry):
            recv[step, me] = outbox[turn, step]
            return carry

        lax.fori_loop(first, end, keep, 0)

    echo_load.wait()
    arrange(0)
    filter_load.wait()
    bins = filt_raw.shape[1]
    bin_ids = lax.broadcasted_iota(jnp.int32, (bins, half), 0)
    d_ids = lax.broadcasted_iota(jnp.int32, (bins, half), 1)
    for s in range(slab_local):
        for e in range(2):
            picker = (bin_ids == (d_ids * 2 + e) * slab_local + s).astype(f32).astype(bf16)
            for part in range(2):
                got = lax.dot_general(
                    filt_raw[part], picker, (((0,), (0,)), ((), ())), preferred_element_type=f32
                )
                filt_all[blk * slab_local + s, part, e] = got.astype(bf16)
    for dz in range(1, blks):
        filter_copy(dz).start()
    for group in range(1, groups):
        arrange(group)

    c_ids = lax.broadcasted_iota(jnp.int32, (outer, half), 0)
    lane_ids = lax.broadcasted_iota(jnp.int32, (8, 2 * half), 1)
    k_ids = jnp.where(lane_ids >= half, (lane_ids - half) * (2 * outer) + outer, lane_ids * (2 * outer))

    def prepare(row, carry):
        shift = shifts_ref[row]
        vr, vi = cosine_sine(c_ids * shift, length)
        vi = -vi
        for part in range(2):
            tr, ti = twist_ref[2 * part], -twist_ref[2 * part + 1]
            rr, ri = cmul(tr, ti, vr, vi)
            inv_twist[row, 2 * part] = rr
            inv_twist[row, 2 * part + 1] = ri
        ur, ui = cosine_sine(k_ids * shift, length)
        ramp[row, 0] = ur
        ramp[row, 1] = -ui
        return carry

    twist_load.wait()
    lax.fori_loop(0, row_count, prepare, 0)
    one_load.wait()
    two_load.wait()

    def lefts(blocks):
        highs, lows = [], []
        for re, im in blocks:
            high, low = split(jnp.concatenate([re, im], 1))
            highs.append(high)
            lows.append(low)
        high, low = jnp.concatenate(highs, 0), jnp.concatenate(lows, 0)
        return jnp.concatenate([high, high, low], 1)

    def forward(step, carry):
        for dt, ds in peers:
            echo_copy(step, dt, ds).wait_recv()
        rows = [recv[step, :, :, i].reshape(2 * outer, 2 * half) for i in range(PAIR)]
        parts = []
        for side in range(2):
            lanes = slice(side * half, (side + 1) * half)
            res = dot(one_ref[side], jnp.concatenate([r[:, lanes] for r in rows], 1))
            parts.append(res[: 2 * outer] + res[2 * outer :])
        total, differ = parts[0] + parts[1], parts[0] - parts[1]
        blocks = []
        for e, value in enumerate((total, differ)):
            tr, ti = twist_ref[2 * e], twist_ref[2 * e + 1]
            for i in range(PAIR):
                lanes = slice(i * half, (i + 1) * half)
                blocks.append(cmul(value[:outer, lanes], value[outer:, lanes], tr, ti))
        spec[step] = dot(lefts(blocks), two_ref[0])
        return carry

    def inverse(step, carry):
        blocks = []
        for e in range(2):
            lanes = slice(e * half, (e + 1) * half)
            for i in range(PAIR):
                row = step * PAIR + i
                picked = filt_all[slabs_ref[row], :, e].astype(f32)
                ur, ui = ramp[row, 0][:1, lanes], ramp[row, 1][:1, lanes]
                gr, gi = cmul(picked[0], picked[1], ur, ui)
                base = (e * PAIR + i) * outer
                z = spec[step, base : base + outer]
                blocks.append(cmul(z[:, :half], z[:, half:], gr, gi))
        back = dot(lefts(blocks), two_ref[1])
        lows, highs = [], []
        for i in range(PAIR):
            row = step * PAIR + i
            got = []
            for e in range(2):
                base = (e * PAIR + i) * outer
                u = back[base : base + outer]
                got.append(
                    cmul(u[:, :half], u[:, half:], inv_twist[row, 2 * e], inv_twist[row, 2 * e + 1])
                )
            lows.append(jnp.concatenate([got[0][0] + got[1][0], got[0][1] + got[1][1]], 0))
            highs.append(jnp.concatenate([got[0][0] - got[1][0], got[0][1] - got[1][1]], 0))
        rows = outer // strips
        for side, value in enumerate((lows, highs)):
            high, low = split(jnp.concatenate(value, 1))
            left = last_ref[side]
            res = dot(left, high)
            res = res[: 2 * rows] + res[2 * rows :] + dot(left[: 2 * rows], low)
            for i in range(PAIR):
                place = lax.rem(step, 8 // PAIR) * PAIR + i + 8 * side
                for part in range(2):
                    out_ref[part, step // (8 // PAIR), pl.ds(place, rows, stride=16), :] = res[
                        part * rows : (part + 1) * rows, i * half : (i + 1) * half
                    ]
        return carry

    def both(step, carry):
        forward(step, 0)
        inverse(step, 0)
        return carry

    early = pairs // 2
    lax.fori_loop(0, early, forward, 0)
    for dz in range(1, blks):
        filter_copy(dz).wait_recv()
        relay_copy(dz).start()
    for dz in range(1, blks):
        relay_copy(dz).wait_recv()
    last_load.wait()
    lax.fori_loop(0, early, inverse, 0)
    lax.fori_loop(early, pairs, both, 0)

    def end_step(step, carry):
        for dt, ds in peers:
            echo_copy(step, dt, ds).wait_send()
        return carry

    lax.fori_loop(0, pairs, end_step, 0)
    for dz in range(1, blks):
        filter_copy(dz).wait_send()
        relay_copy(dz).wait_send()


def per_device(turns, blks, strips, echoes, filters, slab_index, shifts):
    sources = turns * strips
    length = filters.shape[2]
    half = LANES
    outer = length // (2 * half)
    local = outer // sources
    row_count = slab_index.shape[0]
    slab_local = filters.shape[1]
    pairs = row_count // PAIR
    shaped = echoes.reshape(2, -1, 8, 2 * local, half).transpose(0, 1, 3, 2, 4)
    response = filters.reshape(2, slab_local, 2 * outer, half).transpose(0, 2, 1, 3)
    response = response.reshape(2, -1, half)
    tables = [jnp.asarray(t) for t in make_tables(length, sources, strips)]
    hbm, smem = pl.BlockSpec(memory_space=pltpu.HBM), pl.BlockSpec(memory_space=pltpu.SMEM)
    rows = outer // strips
    image = pl.pallas_call(
        functools.partial(body, turns, blks, strips, length),
        out_shape=jax.ShapeDtypeStruct((2, row_count // 8, rows * 16, half), f32),
        in_specs=[smem, smem] + [hbm] * 6,
        out_specs=pl.BlockSpec(memory_space=pltpu.VMEM),
        scratch_shapes=[
            pltpu.VMEM((pairs, sources, 2, PAIR, local, 2 * half), bf16),
            pltpu.VMEM((slab_local * blks, 2, 2, outer, half), bf16),
            pltpu.VMEM((row_count, 4, outer, half), f32),
            pltpu.VMEM((row_count, 2, 8, 2 * half), f32),
            pltpu.VMEM((pairs, 2 * PAIR * outer, 2 * half), f32),
            pltpu.VMEM(tables[0].shape, bf16),
            pltpu.VMEM(tables[1].shape, bf16),
            pltpu.VMEM(tables[2].shape, f32),
            pltpu.VMEM(tables[3].shape[1:], bf16),
            pltpu.VMEM(shaped.shape, bf16),
            pltpu.VMEM(response.shape, bf16),
            pltpu.VMEM((2, 16 * local, half), f32),
            pltpu.VMEM((turns, pairs, 2, PAIR, local, 2 * half), bf16),
            pltpu.SemaphoreType.DMA((pairs, sources)),
            pltpu.SemaphoreType.DMA((pairs, sources)),
            pltpu.SemaphoreType.DMA((blks,)),
            pltpu.SemaphoreType.DMA((blks,)),
            pltpu.SemaphoreType.DMA((blks,)),
            pltpu.SemaphoreType.DMA((blks,)),
            pltpu.SemaphoreType.DMA((6,)),
        ],
        compiler_params=pltpu.CompilerParams(
            collective_id=0, has_side_effects=True, vmem_limit_bytes=56 * 1024 * 1024
        ),
    )(shifts, slab_index, shaped, response, *tables)
    image = image.reshape(2, row_count // 8, rows * 2, 8, half).transpose(0, 1, 3, 2, 4)
    return image.reshape(2, row_count, rows * 2 * half)


def solution(mesh):
    in_specs = (
        P(None, "blk", ("turn", "strip")),
        P(None, "blk", None),
        P(("blk", "turn")),
        P(("blk", "turn")),
    )
    out_specs = P(None, ("blk", "turn"), "strip")
    local = functools.partial(
        per_device, mesh.shape["turn"], mesh.shape["blk"], mesh.shape["strip"]
    )
    return jax.shard_map(local, mesh=mesh, in_specs=in_specs, out_specs=out_specs, check_vma=False)
```

```python
import functools
import math

import jax
import jax.numpy as jnp
import numpy as np
from jax import lax
from jax.experimental import pallas as pl
from jax.experimental.pallas import tpu as pltpu
from jax.sharding import PartitionSpec as P

LANES = 128
PAIR = 2
MESH = pl.DeviceIdType.MESH
f32, bf16 = jnp.float32, jnp.bfloat16


def split_np(table):
    high = table.astype(jnp.bfloat16)
    low = (table - high.astype(np.float64)).astype(jnp.bfloat16)
    return high, low


def make_tables(length, sources, strips):
    half = LANES
    outer = length // (2 * half)
    local = outer // sources
    a_ids, c_ids = np.arange(outer), np.arange(outer)
    b_ids = np.arange(half)
    tau = np.exp(-2j * np.pi * half * c_ids / length)
    first = np.exp(-2j * np.pi * ((c_ids[:, None] * a_ids[None, :]) % outer) / outer)
    stage_one = []
    for mat in (first, tau[:, None] * first):
        grouped = mat.reshape(outer, sources, 1, local)
        top = np.concatenate([grouped.real, -grouped.imag], 2).reshape(outer, 2 * outer)
        bottom = np.concatenate([grouped.imag, grouped.real], 2).reshape(outer, 2 * outer)
        stage_one.append(np.concatenate(split_np(np.concatenate([top, bottom], 0)), 0))
    stage_one = np.stack(stage_one)
    base = np.exp(-2j * np.pi * ((b_ids[:, None] * b_ids[None, :]) % half) / half)

    def right(mat):
        whole = np.concatenate(
            [np.concatenate([mat.real, mat.imag], 1), np.concatenate([-mat.imag, mat.real], 1)], 0
        )
        high, low = split_np(whole)
        return np.concatenate([high, low, high], 0)

    stage_two = np.stack([right(base), right(base.conj())])
    twist = np.exp(-2j * np.pi * ((c_ids[:, None] * b_ids[None, :]) % length) / length)
    omega = np.exp(-2j * np.pi * b_ids / (2 * half))
    turned = twist * omega[None, :]
    twists = np.stack([twist.real, twist.imag, turned.real, turned.imag]).astype(np.float32)
    rows = outer // strips
    last = []
    for strip in range(strips):
        picked = np.arange(strip * rows, (strip + 1) * rows)
        back = np.exp(2j * np.pi * ((picked[:, None] * c_ids[None, :]) % outer) / outer) / length
        per_half = []
        for mat in (back, back * tau.conj()[None, :]):
            whole = np.concatenate(
                [np.concatenate([mat.real, -mat.imag], 1), np.concatenate([mat.imag, mat.real], 1)], 0
            )
            per_half.append(np.concatenate(split_np(whole), 0))
        last.append(np.stack(per_half))
    return stage_one, stage_two, twists, np.stack(last)


def cosine_sine(phase, length):
    quarter = length // 4
    wrapped = phase & (length - 1)
    quadrant = (wrapped + quarter // 2) // quarter if quarter & (quarter - 1) else (
        wrapped + quarter // 2
    ) >> (quarter.bit_length() - 1)
    angle = (wrapped - quadrant * quarter).astype(f32) * (2.0 * math.pi / length)
    square = angle * angle
    sine = angle * (
        1.0 + square * (-1.0 / 6 + square * (1.0 / 120 + square * (-1.0 / 5040 + square * (1.0 / 362880))))
    )
    cosine = 1.0 + square * (
        -0.5
        + square * (1.0 / 24 + square * (-1.0 / 720 + square * (1.0 / 40320 - square * (1.0 / 3628800))))
    )
    odd = (quadrant & 1) == 1
    out_cos = jnp.where(odd, sine, cosine)
    out_sin = jnp.where(odd, cosine, sine)
    quad = quadrant & 3
    out_cos = jnp.where((quad == 1) | (quad == 2), -out_cos, out_cos)
    out_sin = jnp.where(quad >= 2, -out_sin, out_sin)
    return out_cos, out_sin


def cmul(ar, ai, br, bi):
    return ar * br - ai * bi, ar * bi + ai * br


def split(values):
    high = values.astype(bf16)
    return high, (values - high.astype(f32)).astype(bf16)


def dot(left, right):
    return jnp.dot(left, right, preferred_element_type=f32)


def body(
    turns, blks, strips, length,
    shifts_ref, slabs_ref, ech_ref, filt_ref, one_hbm, two_hbm, twist_hbm, last_hbm,
    out_ref,
    recv, filt_all, inv_twist, ramp, spec, one_ref, two_ref, twist_ref, last_ref, ech_raw, filt_raw, staged, outbox,
    send_sem, recv_sem, fsend, frecv, gsend, grecv, load_sem,
):
    turn, blk, strip = lax.axis_index("turn"), lax.axis_index("blk"), lax.axis_index("strip")
    pairs = recv.shape[0]
    row_count = pairs * PAIR
    slab_local = filt_ref.shape[1] * LANES // length
    core = lax.rem(turn, 2)
    partner = turn + 1 - 2 * core
    peers = [(dt, ds) for dt in range(turns) for ds in range(strips) if (dt, ds) != (0, 0)]

    def peer(dt, ds):
        return (lax.rem(turn + dt, turns), blk, lax.rem(strip + ds, strips))

    me = turn * strips + strip
    twist_load = pltpu.make_async_copy(twist_hbm, twist_ref, load_sem.at[0])
    one_load = pltpu.make_async_copy(one_hbm, one_ref, load_sem.at[1])
    two_load = pltpu.make_async_copy(two_hbm, two_ref, load_sem.at[2])
    last_load = pltpu.make_async_copy(last_hbm.at[strip], last_ref, load_sem.at[3])
    echo_load = pltpu.make_async_copy(ech_ref, ech_raw, load_sem.at[4])
    filter_load = pltpu.make_async_copy(filt_ref, filt_raw, load_sem.at[5])
    echo_load.start()
    filter_load.start()

    barrier = pltpu.get_barrier_semaphore()
    for dt, ds in peers:
        pl.semaphore_signal(barrier, inc=1, device_id=peer(dt, ds), device_id_type=MESH)
    for dz in range(1, blks):
        pl.semaphore_signal(
            barrier, inc=1, device_id=(turn, lax.rem(blk + dz, blks), strip), device_id_type=MESH
        )
    twist_load.start()
    one_load.start()
    two_load.start()
    last_load.start()
    pl.semaphore_wait(barrier, len(peers) + blks - 1)

    def echo_copy(step, dt, ds):
        to = peer(dt, ds)
        return pltpu.make_async_remote_copy(
            src_ref=outbox.at[to[0], step],
            dst_ref=recv.at[step, me],
            send_sem=send_sem.at[step, dt * strips + ds],
            recv_sem=recv_sem.at[step, dt * strips + ds],
            device_id=to,
            device_id_type=MESH,
        )

    def filter_copy(dz):
        return pltpu.make_async_remote_copy(
            src_ref=filt_all.at[pl.ds(blk * slab_local, slab_local), core],
            dst_ref=filt_all.at[pl.ds(blk * slab_local, slab_local), core],
            send_sem=fsend.at[dz],
            recv_sem=frecv.at[dz],
            device_id=(turn, lax.rem(blk + dz, blks), strip),
            device_id_type=MESH,
        )

    def relay_copy(dz):
        origin = lax.rem(blk + blks - dz, blks)
        place = filt_all.at[pl.ds(origin * slab_local, slab_local), core]
        return pltpu.make_async_remote_copy(
            src_ref=place,
            dst_ref=place,
            send_sem=gsend.at[dz],
            recv_sem=grecv.at[dz],
            device_id=(partner, blk, strip),
            device_id_type=MESH,
        )

    half = LANES
    outer = length // (2 * half)
    local = ech_raw.shape[2] // 2
    groups = row_count // 8
    per_group = 8 // PAIR

    def arrange(group):
        def fill(to, carry):
            for part in range(2):
                values = ech_raw[part, to * groups + group].astype(f32)
                staged[part] = values.reshape(2 * local * 8, half)
            for part in range(2):
                for row in range(8):
                    for side in range(2):
                        value = staged[part, pl.ds(side * 8 + row, local, stride=16), :]
                        outbox[
                            to, group * per_group + row // PAIR, part, row % PAIR, :,
                            side * half : (side + 1) * half,
                        ] = value.astype(bf16)
            return carry

        lax.fori_loop(0, turns, fill, 0)
        first, end = group * per_group, (group + 1) * per_group

        def start_step(step, carry):
            for dt, ds in peers:
                echo_copy(step, dt, ds).start()
            return carry

        lax.fori_loop(first, end, start_step, 0)

        def keep(step, carry):
            recv[step, me] = outbox[turn, step]
            return carry

        lax.fori_loop(first, end, keep, 0)

    echo_load.wait()
    arrange(0)
    filter_load.wait()
    bins = filt_raw.shape[1]
    bin_ids = lax.broadcasted_iota(jnp.int32, (bins, half), 0)
    d_ids = lax.broadcasted_iota(jnp.int32, (bins, half), 1)
    for s in range(slab_local):
        for e in range(2):
            picker = (bin_ids == (d_ids * 2 + e) * slab_local + s).astype(f32).astype(bf16)
            for part in range(2):
                got = lax.dot_general(
                    filt_raw[part], picker, (((0,), (0,)), ((), ())), preferred_element_type=f32
                )
                filt_all[blk * slab_local + s, part, e] = got.astype(bf16)
    for dz in range(1, blks):
        filter_copy(dz).start()
    for group in range(1, groups):
        arrange(group)

    c_ids = lax.broadcasted_iota(jnp.int32, (outer, half), 0)
    lane_ids = lax.broadcasted_iota(jnp.int32, (8, 2 * half), 1)
    k_ids = jnp.where(lane_ids >= half, (lane_ids - half) * (2 * outer) + outer, lane_ids * (2 * outer))

    def prepare(row, carry):
        shift = shifts_ref[row]
        vr, vi = cosine_sine(c_ids * shift, length)
        vi = -vi
        for part in range(2):
            tr, ti = twist_ref[2 * part], -twist_ref[2 * part + 1]
            rr, ri = cmul(tr, ti, vr, vi)
            inv_twist[row, 2 * part] = rr
            inv_twist[row, 2 * part + 1] = ri
        ur, ui = cosine_sine(k_ids * shift, length)
        ramp[row, 0] = ur
        ramp[row, 1] = -ui
        return carry

    twist_load.wait()
    lax.fori_loop(0, row_count, prepare, 0)
    one_load.wait()
    two_load.wait()

    def lefts(blocks):
        highs, lows = [], []
        for re, im in blocks:
            high, low = split(jnp.concatenate([re, im], 1))
            highs.append(high)
            lows.append(low)
        high, low = jnp.concatenate(highs, 0), jnp.concatenate(lows, 0)
        return jnp.concatenate([high, high, low], 1)

    def forward(step, carry):
        for dt, ds in peers:
            echo_copy(step, dt, ds).wait_recv()
        rows = [recv[step, :, :, i].reshape(2 * outer, 2 * half) for i in range(PAIR)]
        parts = []
        for side in range(2):
            lanes = slice(side * half, (side + 1) * half)
            res = dot(one_ref[side], jnp.concatenate([r[:, lanes] for r in rows], 1))
            parts.append(res[: 2 * outer] + res[2 * outer :])
        total, differ = parts[0] + parts[1], parts[0] - parts[1]
        blocks = []
        for e, value in enumerate((total, differ)):
            tr, ti = twist_ref[2 * e], twist_ref[2 * e + 1]
            for i in range(PAIR):
                lanes = slice(i * half, (i + 1) * half)
                blocks.append(cmul(value[:outer, lanes], value[outer:, lanes], tr, ti))
        spec[step] = dot(lefts(blocks), two_ref[0])
        return carry

    def inverse(step, carry):
        blocks = []
        for e in range(2):
            lanes = slice(e * half, (e + 1) * half)
            for i in range(PAIR):
                row = step * PAIR + i
                picked = filt_all[slabs_ref[row], :, e].astype(f32)
                ur, ui = ramp[row, 0][:1, lanes], ramp[row, 1][:1, lanes]
                gr, gi = cmul(picked[0], picked[1], ur, ui)
                base = (e * PAIR + i) * outer
                z = spec[step, base : base + outer]
                blocks.append(cmul(z[:, :half], z[:, half:], gr, gi))
        back = dot(lefts(blocks), two_ref[1])
        lows, highs = [], []
        for i in range(PAIR):
            row = step * PAIR + i
            got = []
            for e in range(2):
                base = (e * PAIR + i) * outer
                u = back[base : base + outer]
                got.append(
                    cmul(u[:, :half], u[:, half:], inv_twist[row, 2 * e], inv_twist[row, 2 * e + 1])
                )
            lows.append(jnp.concatenate([got[0][0] + got[1][0], got[0][1] + got[1][1]], 0))
            highs.append(jnp.concatenate([got[0][0] - got[1][0], got[0][1] - got[1][1]], 0))
        rows = outer // strips
        for side, value in enumerate((lows, highs)):
            high, low = split(jnp.concatenate(value, 1))
            left = last_ref[side]
            res = dot(left, high)
            res = res[: 2 * rows] + res[2 * rows :] + dot(left[: 2 * rows], low)
            for i in range(PAIR):
                place = lax.rem(step, 8 // PAIR) * PAIR + i + 8 * side
                for part in range(2):
                    out_ref[part, step // (8 // PAIR), pl.ds(place, rows, stride=16), :] = res[
                        part * rows : (part + 1) * rows, i * half : (i + 1) * half
                    ]
        return carry

    def both(step, carry):
        forward(step, 0)
        inverse(step, 0)
        return carry

    early = pairs * 5 // 8
    lax.fori_loop(0, early, forward, 0)
    for dz in range(1, blks):
        filter_copy(dz).wait_recv()
        relay_copy(dz).start()
    for dz in range(1, blks):
        relay_copy(dz).wait_recv()
    last_load.wait()
    lax.fori_loop(0, early, inverse, 0)
    lax.fori_loop(early, pairs, both, 0)

    def end_step(step, carry):
        for dt, ds in peers:
            echo_copy(step, dt, ds).wait_send()
        return carry

    lax.fori_loop(0, pairs, end_step, 0)
    for dz in range(1, blks):
        filter_copy(dz).wait_send()
        relay_copy(dz).wait_send()


def per_device(turns, blks, strips, echoes, filters, slab_index, shifts):
    sources = turns * strips
    length = filters.shape[2]
    half = LANES
    outer = length // (2 * half)
    local = outer // sources
    row_count = slab_index.shape[0]
    slab_local = filters.shape[1]
    pairs = row_count // PAIR
    shaped = echoes.reshape(2, -1, 8, 2 * local, half).transpose(0, 1, 3, 2, 4)
    response = filters.reshape(2, slab_local, 2 * outer, half).transpose(0, 2, 1, 3)
    response = response.reshape(2, -1, half)
    tables = [jnp.asarray(t) for t in make_tables(length, sources, strips)]
    hbm, smem = pl.BlockSpec(memory_space=pltpu.HBM), pl.BlockSpec(memory_space=pltpu.SMEM)
    rows = outer // strips
    image = pl.pallas_call(
        functools.partial(body, turns, blks, strips, length),
        out_shape=jax.ShapeDtypeStruct((2, row_count // 8, rows * 16, half), f32),
        in_specs=[smem, smem] + [hbm] * 6,
        out_specs=pl.BlockSpec(memory_space=pltpu.VMEM),
        scratch_shapes=[
            pltpu.VMEM((pairs, sources, 2, PAIR, local, 2 * half), bf16),
            pltpu.VMEM((slab_local * blks, 2, 2, outer, half), bf16),
            pltpu.VMEM((row_count, 4, outer, half), f32),
            pltpu.VMEM((row_count, 2, 8, 2 * half), f32),
            pltpu.VMEM((pairs, 2 * PAIR * outer, 2 * half), f32),
            pltpu.VMEM(tables[0].shape, bf16),
            pltpu.VMEM(tables[1].shape, bf16),
            pltpu.VMEM(tables[2].shape, f32),
            pltpu.VMEM(tables[3].shape[1:], bf16),
            pltpu.VMEM(shaped.shape, bf16),
            pltpu.VMEM(response.shape, bf16),
            pltpu.VMEM((2, 16 * local, half), f32),
            pltpu.VMEM((turns, pairs, 2, PAIR, local, 2 * half), bf16),
            pltpu.SemaphoreType.DMA((pairs, sources)),
            pltpu.SemaphoreType.DMA((pairs, sources)),
            pltpu.SemaphoreType.DMA((blks,)),
            pltpu.SemaphoreType.DMA((blks,)),
            pltpu.SemaphoreType.DMA((blks,)),
            pltpu.SemaphoreType.DMA((blks,)),
            pltpu.SemaphoreType.DMA((6,)),
        ],
        compiler_params=pltpu.CompilerParams(
            collective_id=0, has_side_effects=True, vmem_limit_bytes=56 * 1024 * 1024
        ),
    )(shifts, slab_index, shaped, response, *tables)
    image = image.reshape(2, row_count // 8, rows * 2, 8, half).transpose(0, 1, 3, 2, 4)
    return image.reshape(2, row_count, rows * 2 * half)


def solution(mesh):
    in_specs = (
        P(None, "blk", ("turn", "strip")),
        P(None, "blk", None),
        P(("blk", "turn")),
        P(("blk", "turn")),
    )
    out_specs = P(None, ("blk", "turn"), "strip")
    local = functools.partial(
        per_device, mesh.shape["turn"], mesh.shape["blk"], mesh.shape["strip"]
    )
    return jax.shard_map(local, mesh=mesh, in_specs=in_specs, out_specs=out_specs, check_vma=False)
```
